32 devices in a mesh: tm: 8 (over z, x), env: 4 (over y, core).
Axes of the slice: x: 2, y: 2, z: 4, core: 2. Of those that a mesh axis runs over, the one named last changes fastest.
Arguments:
- features: bfloat16 [512, 64, 4096], P('tm', 'env'), may hold values from -6 to 6
- w_hidden: bfloat16 [4096, 1024], P('tm'), may hold values from -0.09375 to 0.09375
- b_hidden: float32 [1024], replicated, may hold values from -3 to 3
- w_value: float32 [1024], replicated, may hold values from -0.1875 to 0.1875
- w_policy: bfloat16 [4096, 256], P('tm'), may hold values from -15.0625 to 15.0625
- old_value: float32 [512, 64], P('tm', 'env'), may hold values from -6 to 6
- rewards: float32 [512, 64], P('tm', 'env'), may hold values from -0.3 to 0.3
- dones: int32 [512, 64], P('tm', 'env'), may hold values 0 or 1
- discounts: float32 [2, 64], P(None, 'env'), may hold values from 0.98333333 to 1, as said below
- last_value: float32 [64], P('env'), may hold values from -6 to 6
- actions: int32 [512, 64], P('tm', 'env'), may hold values from 0 to 255
- old_logprob: float32 [512, 64], P('tm', 'env'), may hold values from -7 to -4.5
Outputs:
- norm_adv: float32 [512, 64], P('tm', 'env')
- value_pred: float32 [512, 64], P('tm', 'env')
- new_logprob: float32 [512, 64], P('tm', 'env')
- losses: float32 [2], replicated
The draws below stay inside these ranges and needn't reach their ends.
Inputs may be any that keep to these rules, and one draw needn't show every extreme that they name: `discounts`: every entry is below 1.
All inputs are finite; a program needn't handle non-finite values. No bound on the sum of `dones` on one device may be relied on, other than what follows from the above.
Results may differ from the reference program's by a relative error of at most 0.0003.
Values may be sent and summed in bfloat16 or wider, within the bound.
A program may use at most 64 MiB of HBM per device.

```python
import math
import jax
import jax.numpy as jnp
from jax import lax

F = 4096
H = 1024
A = 256
TC = 64
TIME = 512
ENVS = 64


def draw_discounts(key, part):
    keys = jax.random.split(jax.random.fold_in(key, 17), 5)
    share = 0.5
    longer = jax.random.uniform(keys[0], (ENVS,)) < share
    long_lo = math.log(0.05 / TIME)
    long_hi = math.log(1.0 / TIME)
    short_lo = math.log(1.0 / 100.0)
    short_hi = math.log(1.0 / 60.0)

    def pick(first, second):
        upper = jnp.exp(long_lo + jax.random.uniform(first, (ENVS,)) * (long_hi - long_lo))
        lower = jnp.exp(short_lo + jax.random.uniform(second, (ENVS,)) * (short_hi - short_lo))
        return 1.0 - jnp.where(longer, upper, lower)
    return jnp.stack([pick(keys[1], keys[2]), pick(keys[3], keys[4])]).astype(jnp.float32)


def draw_w_policy(key, part):
    keys = jax.random.split(jax.random.fold_in(key, 29), 2)
    base = jax.random.truncated_normal(keys[0], -6.0, 6.0, (F, A), jnp.float32) * F ** (-0.5)
    return base.astype(jnp.bfloat16)


def plant(entries, stream_key, least, largest):
    longest = entries.shape.index(max(entries.shape))
    spots = []
    for shift in (0, 1):
        where = [jax.random.randint(jax.random.fold_in(stream_key, axis), (), 0, length) for axis, length in enumerate(entries.shape)]
        where[longest] = (where[longest] + shift) % entries.shape[longest]
        spots.append(tuple(where))
    return entries.at[spots[0]].set(least).at[spots[1]].set(largest)


def block_scale(own_key, shape, cuts, low, high):
    gain = 1.0
    for dim, shards_of in cuts:
        heights = jax.random.uniform(jax.random.fold_in(jax.random.fold_in(own_key, 6), dim), (shards_of,), jnp.float32, low / len(cuts), high / len(cuts))
        gain = gain * jnp.repeat(jnp.exp(heights), shape[dim] // shards_of).reshape((-1,) + (1,) * (len(shape) - 1 - dim))
    return gain


def normal_values(own_key, extent, deviation, most, pieces=(), dtype=jnp.bfloat16):
    gain = block_scale(own_key, extent, pieces, -0.22, 0.18) if pieces else 1.0
    array = jax.random.normal(own_key, extent, jnp.float32) * deviation * gain
    return jnp.minimum(jnp.maximum(array, -most), most).astype(dtype)


def setup_inputs(seed: int = 0) -> dict:
    key_of = jax.random.split(jax.random.key(seed), 13)
    return {
        "features": normal_values(key_of[0], (TIME, ENVS, F), 1.0, 6.0, ((0, 8), (1, 4))),
        "w_hidden": normal_values(key_of[1], (F, H), F ** -0.5, 0.09375, ((0, 8),)),
        "b_hidden": normal_values(key_of[2], (H,), 0.5, 3.0, (), jnp.float32),
        "w_value": normal_values(key_of[3], (H,), H ** -0.5, 0.1875, (), jnp.float32),
        "w_policy": draw_w_policy(jax.random.fold_in(key_of[12], 71), 0),
        "old_value": normal_values(key_of[5], (TIME, ENVS), 1.0, 6.0, ((0, 8), (1, 4)), jnp.float32),
        "rewards": normal_values(key_of[6], (TIME, ENVS), 0.05, 0.3, ((0, 8), (1, 4)), jnp.float32),
        "dones": plant((jax.random.randint(key_of[7], (TIME, ENVS), 0, 4 * TIME) < 1).astype(jnp.int32), jax.random.fold_in(key_of[7], 1), 0, 1),
        "discounts": draw_discounts(jax.random.fold_in(key_of[12], 71), 0),
        "last_value": normal_values(key_of[9], (ENVS,), 1.0, 6.0, ((0, 4),), jnp.float32),
        "actions": plant(jax.random.randint(key_of[10], (TIME, ENVS), 0, A), jax.random.fold_in(key_of[10], 1), 0, A - 1).astype(jnp.int32),
        "old_logprob": jnp.clip(-7.0 + 2.5 * jax.random.uniform(key_of[11], (TIME, ENVS), jnp.float32) ** block_scale(key_of[11], (TIME, ENVS), ((0, 8), (1, 4)), -0.2, 0.2), -7.0, -4.5),
    }


def reference(features, w_hidden, b_hidden, w_value, w_policy, old_value, rewards, dones, discounts, last_value, actions, old_logprob):
    blocks = TIME // TC
    feat = features.reshape(blocks, TC * ENVS, F)
    acts = actions.reshape(blocks, TC * ENVS)

    def heads(item):
        rows, taken = item
        pre = jnp.dot(rows, w_hidden, preferred_element_type=jnp.float32) + b_hidden
        hidden_act = jnp.tanh(pre)
        value = jnp.dot(hidden_act, w_value, precision=lax.Precision.HIGHEST)
        logits = jnp.dot(rows, w_policy, preferred_element_type=jnp.float32)
        logp = jax.nn.log_softmax(logits, axis=-1)
        picked = jnp.take_along_axis(logp, taken[:, None].astype(jnp.int32), axis=1)[:, 0]
        return (value, picked)
    values, picked = lax.map(heads, (feat, acts))
    value_pred = values.reshape(TIME, ENVS)
    new_logprob = picked.reshape(TIME, ENVS)
    keep = 1.0 - dones.astype(jnp.float32)
    gamma = discounts[0]
    lam = discounts[1]
    next_value = jnp.concatenate([old_value[1:], last_value[None]], 0)
    delta = rewards + gamma * keep * next_value - old_value

    def backward(carry, item):
        step_delta, step_keep = item
        adv = step_delta + gamma * lam * step_keep * carry
        return (adv, adv)
    _, advantage = lax.scan(backward, jnp.zeros((ENVS,), jnp.float32), (delta, keep), reverse=True)
    count = TIME * ENVS
    adv_mean = jnp.sum(advantage) / count
    adv_var = jnp.sum(advantage * advantage) / count - adv_mean * adv_mean
    norm_adv = (advantage - adv_mean) / jnp.sqrt(adv_var + 0.25)
    ratio = jnp.exp(new_logprob - old_logprob)
    policy_term = -jnp.minimum(ratio * norm_adv, jnp.clip(ratio, 0.8, 1.2) * norm_adv)
    returns = advantage + old_value
    clipped = old_value + jnp.clip(value_pred - old_value, -0.2, 0.2)
    value_term = 0.5 * jnp.maximum((value_pred - returns) ** 2, (clipped - returns) ** 2)
    losses = jnp.stack([jnp.sum(policy_term), jnp.sum(value_term)]) / count
    return (norm_adv, value_pred, new_logprob, losses)
```

```python
import functools

import jax
import jax.numpy as jnp
from jax import lax
from jax.experimental import pallas as pl
from jax.experimental.pallas import tpu as pltpu
from jax.sharding import PartitionSpec as P

MESH = pl.DeviceIdType.MESH
CORES = 2


def along_x(tm):
    nx = 1
    while (2 * nx) * (2 * nx) <= tm and tm % (2 * nx) == 0:
        nx *= 2
    return nx


def loop(count, body):
    if count == 1:
        body(0)
    elif count > 1:
        lax.fori_loop(0, count, lambda i, _: (body(i), 0)[1], 0)


def later(x, s, fill):
    return jnp.concatenate([x[s:], jnp.full((s, x.shape[1]), fill, x.dtype)], 0)


def kernel(
    sizes,
    feat_hbm,
    wh_hbm,
    wp_hbm,
    bias_ref,
    wv_ref,
    old_ref,
    rew_ref,
    done_ref,
    disc_ref,
    last_ref,
    act_ref,
    olp_ref,
    norm_ref,
    value_ref,
    logp_ref,
    loss_ref,
    feat,
    wa,
    wb,
    acca,
    accb,
    chain,
    stat,
    lsum,
    feat_sem,
    w_sem,
    recva,
    recvb,
    senda,
    sendb,
    chain_send,
    chain_recv,
    stat_send,
    stat_recv,
    lsum_send,
    lsum_recv,
):
    tmn, envn, steps, envs, shard, hid, acts = sizes
    nx = along_x(tmn)
    nz = tmn // nx
    ny = envn // CORES
    piece = shard // envn
    rows = steps * envs
    ca = wa.shape[1]
    ch = hid - ca
    n = tmn * envn
    ti = lax.axis_index("tm")
    ei = lax.axis_index("env")
    z, x = ti // nx, ti % nx
    y, c = ei // CORES, ei % CORES
    me = ti * envn + ei

    loads = [
        pltpu.make_async_copy(
            wh_hbm.at[:, pl.ds(0, ca)], wa.at[pl.ds(ti * shard, shard), :], w_sem.at[0]
        ),
        pltpu.make_async_copy(
            wh_hbm.at[:, pl.ds(ca, ch)],
            wb.at[pl.ds(ti * shard, shard), pl.ds(0, ch)],
            w_sem.at[1],
        ),
        pltpu.make_async_copy(
            wp_hbm, wb.at[pl.ds(ti * shard, shard), pl.ds(ch, acts)], w_sem.at[2]
        ),
    ]
    for load in loads:
        load.start()
    fetch = pltpu.make_async_copy(feat_hbm, feat, feat_sem)
    fetch.start()

    barrier = pltpu.get_barrier_semaphore()

    def greet(k):
        other = (me + 1 + k) % n
        pl.semaphore_signal(
            barrier,
            inc=1,
            device_id={"tm": other // envn, "env": other % envn},
            device_id_type=MESH,
        )

    loop(n - 1, greet)

    keep = 1.0 - done_ref[...].astype(jnp.float32)
    old = old_ref[...]
    gamma = disc_ref[0:1, :]
    lam = disc_ref[1:2, :]
    row = lax.broadcasted_iota(jnp.int32, (steps, envs), 0)
    gain = (gamma * lam) * keep
    base = rew_ref[...] + gamma * keep * later(old, 1, 0.0) - old
    tail = jnp.where(row == steps - 1, gamma * keep, 0.0)
    s = 1
    while s < steps:
        base = base + gain * later(base, s, 0.0)
        tail = tail + gain * later(tail, s, 0.0)
        gain = gain * later(gain, s, 1.0)
        s *= 2
    chain[ti, 0:1, 0:envs] = gain[0:1]
    chain[ti, 1:2, 0:envs] = base[0:1]
    chain[ti, 2:3, 0:envs] = tail[0:1]
    chain[ti, 3:4, 0:envs] = old[0:1]

    for load in loads:
        load.wait()
    pl.semaphore_wait(barrier, n - 1)

    def tell_chain(k):
        pltpu.make_async_remote_copy(
            src_ref=chain.at[ti],
            dst_ref=chain.at[ti],
            send_sem=chain_send,
            recv_sem=chain_recv,
            device_id={"tm": (ti + 1 + k) % tmn, "env": ei},
            device_id_type=MESH,
        ).start()

    loop(tmn - 1, tell_chain)

    def tell_all(buf, send_sem, recv_sem):
        def go(k):
            other = (me + 1 + k) % n
            pltpu.make_async_remote_copy(
                src_ref=buf.at[me],
                dst_ref=buf.at[me],
                send_sem=send_sem,
                recv_sem=recv_sem,
                device_id={"tm": other // envn, "env": other % envn},
                device_id_type=MESH,
            ).start()

        loop(n - 1, go)

    def took(buf, count, sem):
        pltpu.make_async_copy(buf.at[pl.ds(0, count)], buf.at[pl.ds(0, count)], sem).wait()

    def part(w, pz, px, py, pc):
        start = (pz * nx + px) * shard + (py * CORES + pc) * piece
        return w.at[pl.ds(pl.multiple_of(start, piece), piece), :]

    def slot(pz, px, py, pc):
        return (pz * nx + px) * envn + py * CORES + pc

    groups = {"a": (wa, recva, senda), "b": (wb, recvb, sendb)}

    def send(g, pz, px, py, dz, dx, dy, dc):
        w, recv, out = groups[g]
        block = part(w, pz, px, py, c)
        pltpu.make_async_remote_copy(
            src_ref=block,
            dst_ref=block,
            send_sem=out,
            recv_sem=recv.at[slot(pz, px, py, c)],
            device_id={
                "tm": ((z + dz) % nz) * nx + (x + dx) % nx,
                "env": ((y + dy) % ny) * CORES + (c + dc) % CORES,
            },
            device_id_type=MESH,
        ).start()

    def wait(g, pz, px, py, pc):
        w, recv, _ = groups[g]
        block = part(w, pz, px, py, pc)
        pltpu.make_async_copy(block, block, recv.at[slot(pz, px, py, pc)]).wait()

    def to_z(g, pz, px, py):
        loop(nz - 1, lambda k: send(g, pz, px, py, k + 1, 0, 0, 0))

    def to_x(g, pz, px, py):
        loop(nx - 1, lambda k: send(g, pz, px, py, 0, k + 1, 0, 0))

    def to_y(g, pz, px, py):
        loop(ny - 1, lambda k: send(g, pz, px, py, 0, 0, k + 1, 0))

    def to_core(g, pz, px, py):
        send(g, pz, px, py, 0, 0, 0, 1)

    tile = 256

    def multiply(g, start, depth, first=False):
        w = groups[g][0]
        acc = acca if g == "a" else accb
        k = pl.ds(pl.multiple_of(start, depth), depth)

        def at(i):
            r = pl.ds(pl.multiple_of(i * tile, tile), tile)
            new = jnp.dot(feat[r, k], w[k, :], preferred_element_type=jnp.float32)
            acc[r, :] = new if first else acc[r, :] + new

        loop(rows // tile, at)

    depth = shard // ny
    fine = depth % 128 == 0

    def settle(g, pz, px, py):
        wait(g, pz, px, py, (c + 1) % CORES)
        if fine:
            multiply(g, (pz * nx + px) * shard + py * depth, depth)

    to_x("b", z, x, y)
    to_z("a", z, x, y)
    to_z("b", z, x, y)
    loop(ny, lambda k: to_x("a", z, x, (y + k) % ny))

    fetch.wait()
    multiply("b", ti * shard, shard, True)

    def b1(k):
        px = (x + 1 + k) % nx
        wait("b", z, px, y, c)
        to_z("b", z, px, y)
        to_y("b", z, px, y)
        to_core("b", z, px, y)

    loop(nx - 1, b1)
    multiply("a", ti * shard, shard, True)
    loop(nx - 1, lambda k: settle("b", z, (x + 1 + k) % nx, y))

    def first_z(k):
        pz = (z + 1 + k) % nz
        wait("a", pz, x, y, c)
        to_y("a", pz, x, y)
        to_x("a", pz, x, y)
        to_core("a", pz, x, y)
        wait("b", pz, x, y, c)
        to_y("b", pz, x, y)
        to_core("b", pz, x, y)
        settle("a", pz, x, y)
        settle("b", pz, x, y)

    loop(nz - 1, first_z)

    took(chain, tmn - 1, chain_recv)

    def back(k, state):
        carry, value_after = state
        at = tmn - 1 - k
        blk = chain[at]
        new = blk[1:2, 0:envs] + blk[2:3, 0:envs] * value_after + blk[0:1, 0:envs] * carry
        reached = at > ti
        return (
            jnp.where(reached, new, carry),
            jnp.where(reached, blk[3:4, 0:envs], value_after),
        )

    carry, value_after = lax.fori_loop(
        0, tmn, back, (jnp.zeros((1, envs), jnp.float32), last_ref[...])
    )
    advantage = base + tail * value_after + gain * carry
    stat[me, 0:1, 0:envs] = jnp.sum(advantage, axis=0, keepdims=True)
    stat[me, 1:2, 0:envs] = jnp.sum(advantage * advantage, axis=0, keepdims=True)
    norm_ref[...] = advantage
    tell_all(stat, stat_send, stat_recv)

    def own_x(k):
        px, py = (x + 1 + k // ny) % nx, (y + k % ny) % ny
        wait("a", z, px, py, c)
        to_core("a", z, px, py)
        settle("a", z, px, py)

    def far_b(k):
        pz, px = (z + 1 + k // (nx - 1)) % nz, (x + 1 + k % (nx - 1)) % nx
        wait("b", pz, px, y, c)
        to_y("b", pz, px, y)
        to_core("b", pz, px, y)
        settle("b", pz, px, y)

    def near_y(k):
        pz, py = (z + 1 + k // (ny - 1)) % nz, (y + 1 + k % (ny - 1)) % ny
        wait("a", pz, x, py, c)
        to_x("a", pz, x, py)
        to_core("a", pz, x, py)
        settle("a", pz, x, py)

    def last_b(k):
        sh, py = 1 + k // (ny - 1), (y + 1 + k % (ny - 1)) % ny
        pz, px = (z + sh // nx) % nz, (x + sh % nx) % nx
        wait("b", pz, px, py, c)
        to_core("b", pz, px, py)
        settle("b", pz, px, py)

    def last_a(k):
        pz = (z + 1 + k // (ny * (nx - 1))) % nz
        px = (x + 1 + (k // ny) % (nx - 1)) % nx
        py = (y + k % ny) % ny
        wait("a", pz, px, py, c)
        to_core("a", pz, px, py)
        settle("a", pz, px, py)

    loop((nz - 1) * (ny - 1), near_y)
    loop((nx - 1) * ny, own_x)
    if nx > 1:
        loop((nz - 1) * (nx - 1), far_b)
    loop((nz * nx - 1) * (ny - 1), last_b)
    if nx > 1:
        loop((nz - 1) * (nx - 1) * ny, last_a)

    if not fine:

        def rest(k):
            start = ((ti + 1 + k) % tmn) * shard
            multiply("a", start, shard)
            multiply("b", start, shard)

        loop(tmn - 1, rest)

    took(stat, n - 1, stat_recv)
    count = rows * n
    adv_mean = jnp.sum(stat[:, 0:1, 0:envs]) / count
    adv_var = jnp.sum(stat[:, 1:2, 0:envs]) / count - adv_mean * adv_mean

    span = tile // envs

    def finish(i):
        r = pl.ds(pl.multiple_of(i * tile, tile), tile)
        t = pl.ds(pl.multiple_of(i * span, span), span)
        cube = (span, envs, envs)
        diag = lax.broadcasted_iota(jnp.int32, cube, 1) == lax.broadcasted_iota(jnp.int32, cube, 2)

        def square(col):
            return jnp.sum(jnp.where(diag, col.reshape(span, envs, 1), 0.0), axis=1)

        taken = act_ref[t, :].astype(jnp.float32)
        taken = jnp.sum(jnp.where(diag, taken[:, None, :], 0.0), axis=2, keepdims=True)
        taken = taken.reshape(tile, 1).astype(jnp.int32)
        logits = accb[r, ch : ch + acts]
        top = jnp.max(logits, axis=1, keepdims=True)
        total = jnp.sum(jnp.exp(logits - top), axis=1, keepdims=True)
        choose = lax.broadcasted_iota(jnp.int32, (tile, acts), 1) == taken
        picked = jnp.sum(jnp.where(choose, logits - top, 0.0), axis=1, keepdims=True)
        logp_ref[t, :] = square(picked - jnp.log(total))
        front = jnp.tanh(acca[r, :] + bias_ref[:, 0:ca]) * wv_ref[:, 0:ca]
        behind = jnp.tanh(accb[r, 0:ch] + bias_ref[:, ca:hid]) * wv_ref[:, ca:hid]
        value = jnp.sum(front, axis=1, keepdims=True) + jnp.sum(behind, axis=1, keepdims=True)
        value_ref[t, :] = square(value)

    loop(rows // tile, finish)

    advantage = norm_ref[...]
    norm = (advantage - adv_mean) / jnp.sqrt(jnp.full((1, 1), adv_var + 0.25))
    norm_ref[...] = norm
    old = old_ref[...]
    value_pred = value_ref[...]
    ratio = jnp.exp(logp_ref[...] - olp_ref[...])
    policy_term = -jnp.minimum(ratio * norm, jnp.clip(ratio, 0.8, 1.2) * norm)
    returns = advantage + old
    clipped = old + jnp.clip(value_pred - old, -0.2, 0.2)
    value_term = 0.5 * jnp.maximum((value_pred - returns) ** 2, (clipped - returns) ** 2)
    lsum[me, 0:1, 0:envs] = jnp.sum(policy_term, axis=0, keepdims=True)
    lsum[me, 1:2, 0:envs] = jnp.sum(value_term, axis=0, keepdims=True)
    tell_all(lsum, lsum_send, lsum_recv)

    sent_a = (
        (nz - 1)
        + (nx - 1) * ny
        + (nz - 1) * (ny - 1 + nx)
        + (nz - 1) * (ny - 1) * nx
        + nz * (nx - 1) * ny
    )
    sent_b = (
        (nx - 1)
        + (nz - 1)
        + (nx - 1) * (nz - 1 + ny)
        + (nz - 1) * nx * ny
        + (nz * nx - 1) * (ny - 1)
    )

    def drain(g, count):
        w, _, out = groups[g]
        block = w.at[pl.ds(0, piece), :]
        loop(count, lambda k: pltpu.make_async_copy(block, block, out).wait())

    drain("a", sent_a)
    drain("b", sent_b)
    took(chain, tmn - 1, chain_send)
    took(stat, n - 1, stat_send)
    took(lsum, n - 1, lsum_recv)
    loss_ref[0] = jnp.sum(lsum[:, 0:1, 0:envs]) / count
    loss_ref[1] = jnp.sum(lsum[:, 1:2, 0:envs]) / count
    took(lsum, n - 1, lsum_send)


def solution(mesh):
    tmn, envn = mesh.shape["tm"], mesh.shape["env"]

    def shards(
        features,
        w_hidden,
        b_hidden,
        w_value,
        w_policy,
        old_value,
        rewards,
        dones,
        discounts,
        last_value,
        actions,
        old_logprob,
    ):
        steps, envs, width = features.shape
        shard, hid = w_hidden.shape
        acts = w_policy.shape[1]
        rows = steps * envs
        n = tmn * envn
        ca = hid * 3 // 4
        cb = hid - ca + acts
        sizes = (tmn, envn, steps, envs, shard, hid, acts)
        cell = jax.ShapeDtypeStruct((steps, envs), jnp.float32)
        vmem = pl.BlockSpec(memory_space=pltpu.VMEM)
        dma = pltpu.SemaphoreType.DMA
        return pl.pallas_call(
            functools.partial(kernel, sizes),
            out_shape=(cell, cell, cell, jax.ShapeDtypeStruct((2,), jnp.float32)),
            in_specs=[pl.BlockSpec(memory_space=pl.ANY)] * 3 + [vmem] * 9,
            out_specs=(vmem, vmem, vmem, pl.BlockSpec(memory_space=pltpu.SMEM)),
            scratch_shapes=[
                pltpu.VMEM((rows, width), jnp.bfloat16),
                pltpu.VMEM((width, ca), jnp.bfloat16),
                pltpu.VMEM((width, cb), jnp.bfloat16),
                pltpu.VMEM((rows, ca), jnp.float32),
                pltpu.VMEM((rows, cb), jnp.float32),
                pltpu.VMEM((tmn, 8, 128), jnp.float32),
                pltpu.VMEM((n, 8, 128), jnp.float32),
                pltpu.VMEM((n, 8, 128), jnp.float32),
                dma,
                dma((3,)),
                dma((n,)),
                dma((n,)),
                dma,
                dma,
                dma,
                dma,
                dma,
                dma,
                dma,
                dma,
            ],
            compiler_params=pltpu.CompilerParams(
                collective_id=0, has_side_effects=True, vmem_limit_bytes=60 * 1024 * 1024
            ),
        )(
            features.reshape(rows, width),
            w_hidden,
            w_policy,
            b_hidden.reshape(1, hid),
            w_value.reshape(1, hid),
            old_value,
            rewards,
            dones,
            discounts,
            last_value.reshape(1, envs),
            actions,
            old_logprob,
        )

    in_specs = (
        P("tm", "env", None),
        P("tm", None),
        P(),
        P(),
        P("tm", None),
        P("tm", "env"),
        P("tm", "env"),
        P("tm", "env"),
        P(None, "env"),
        P("env"),
        P("tm", "env"),
        P("tm", "env"),
    )
    out_specs = (P("tm", "env"), P("tm", "env"), P("tm", "env"), P())
    return jax.shard_map(shards, mesh=mesh, in_specs=in_specs, out_specs=out_specs, check_vma=False)
```

```python
import functools

import jax
import jax.numpy as jnp
from jax import lax
from jax.experimental import pallas as pl
from jax.experimental.pallas import tpu as pltpu
from jax.sharding import PartitionSpec as P

MESH = pl.DeviceIdType.MESH
CORES = 2


def along_x(tm):
    nx = 1
    while (2 * nx) * (2 * nx) <= tm and tm % (2 * nx) == 0:
        nx *= 2
    return nx


def loop(count, body):
    if count == 1:
        body(0)
    elif count > 1:
        lax.fori_loop(0, count, lambda i, _: (body(i), 0)[1], 0)


def later(x, s, fill):
    return jnp.concatenate([x[s:], jnp.full((s, x.shape[1]), fill, x.dtype)], 0)


def kernel(
    sizes,
    feat_hbm,
    wh_hbm,
    wp_hbm,
    bias_ref,
    wv_ref,
    old_t,
    rew_t,
    done_t,
    disc_ref,
    last_ref,
    act_t,
    olp_t,
    norm_out,
    value_out,
    logp_out,
    loss_ref,
    norm_ref,
    value_ref,
    logp_ref,
    act_ref,
    feat,
    wa,
    wb,
    acca,
    accb,
    chain,
    stat,
    lsum,
    feat_sem,
    w_sem,
    recva,
    recvb,
    senda,
    sendb,
    chain_send,
    chain_recv,
    stat_send,
    stat_recv,
    lsum_send,
    lsum_recv,
):
    tmn, envn, steps, envs, shard, hid, acts = sizes
    nx = along_x(tmn)
    nz = tmn // nx
    ny = envn // CORES
    piece = shard // envn
    rows = steps * envs
    ca = wa.shape[1]
    ch = hid - ca
    n = tmn * envn
    ti = lax.axis_index("tm")
    ei = lax.axis_index("env")
    z, x = ti // nx, ti % nx
    y, c = ei // CORES, ei % CORES
    me = ti * envn + ei

    loads = [
        pltpu.make_async_copy(
            wh_hbm.at[:, pl.ds(0, ca)], wa.at[pl.ds(ti * shard, shard), :], w_sem.at[0]
        ),
        pltpu.make_async_copy(
            wh_hbm.at[:, pl.ds(ca, ch)],
            wb.at[pl.ds(ti * shard, shard), pl.ds(0, ch)],
            w_sem.at[1],
        ),
        pltpu.make_async_copy(
            wp_hbm, wb.at[pl.ds(ti * shard, shard), pl.ds(ch, acts)], w_sem.at[2]
        ),
    ]
    for load in loads:
        load.start()
    fetch = pltpu.make_async_copy(feat_hbm, feat, feat_sem)
    fetch.start()

    barrier = pltpu.get_barrier_semaphore()

    def greet(k):
        other = (me + 1 + k) % n
        pl.semaphore_signal(
            barrier,
            inc=1,
            device_id={"tm": other // envn, "env": other % envn},
            device_id_type=MESH,
        )

    loop(n - 1, greet)

    keep = 1.0 - done_t[...].astype(jnp.float32).T
    old = old_t[...].T
    gamma = disc_ref[0:1, :]
    lam = disc_ref[1:2, :]
    row = lax.broadcasted_iota(jnp.int32, (steps, envs), 0)
    gain = (gamma * lam) * keep
    base = rew_t[...].T + gamma * keep * later(old, 1, 0.0) - old
    tail = jnp.where(row == steps - 1, gamma * keep, 0.0)
    s = 1
    while s < steps:
        base = base + gain * later(base, s, 0.0)
        tail = tail + gain * later(tail, s, 0.0)
        gain = gain * later(gain, s, 1.0)
        s *= 2
    act_ref[...] = act_t[...].astype(jnp.float32).T
    chain[ti, 0:1, 0:envs] = gain[0:1]
    chain[ti, 1:2, 0:envs] = base[0:1]
    chain[ti, 2:3, 0:envs] = tail[0:1]
    chain[ti, 3:4, 0:envs] = old[0:1]

    for load in loads:
        load.wait()
    pl.semaphore_wait(barrier, n - 1)

    def tell_chain(k):
        pltpu.make_async_remote_copy(
            src_ref=chain.at[ti],
            dst_ref=chain.at[ti],
            send_sem=chain_send,
            recv_sem=chain_recv,
            device_id={"tm": (ti + 1 + k) % tmn, "env": ei},
            device_id_type=MESH,
        ).start()

    loop(tmn - 1, tell_chain)

    def tell_all(buf, send_sem, recv_sem):
        def go(k):
            other = (me + 1 + k) % n
            pltpu.make_async_remote_copy(
                src_ref=buf.at[me],
                dst_ref=buf.at[me],
                send_sem=send_sem,
                recv_sem=recv_sem,
                device_id={"tm": other // envn, "env": other % envn},
                device_id_type=MESH,
            ).start()

        loop(n - 1, go)

    def took(buf, count, sem):
        pltpu.make_async_copy(buf.at[pl.ds(0, count)], buf.at[pl.ds(0, count)], sem).wait()

    def part(w, pz, px, py, pc):
        start = (pz * nx + px) * shard + (py * CORES + pc) * piece
        return w.at[pl.ds(pl.multiple_of(start, piece), piece), :]

    def slot(pz, px, py, pc):
        return (pz * nx + px) * envn + py * CORES + pc

    groups = {"a": (wa, recva, senda), "b": (wb, recvb, sendb)}

    def send(g, pz, px, py, dz, dx, dy, dc):
        w, recv, out = groups[g]
        block = part(w, pz, px, py, c)
        pltpu.make_async_remote_copy(
            src_ref=block,
            dst_ref=block,
            send_sem=out,
            recv_sem=recv.at[slot(pz, px, py, c)],
            device_id={
                "tm": ((z + dz) % nz) * nx + (x + dx) % nx,
                "env": ((y + dy) % ny) * CORES + (c + dc) % CORES,
            },
            device_id_type=MESH,
        ).start()

    def wait(g, pz, px, py, pc):
        w, recv, _ = groups[g]
        block = part(w, pz, px, py, pc)
        pltpu.make_async_copy(block, block, recv.at[slot(pz, px, py, pc)]).wait()

    def to_z(g, pz, up):
        there = z + 1 < nz if up else z > 0

        @pl.when(there)
        def _():
            send(g, pz, x, y, 1 if up else nz - 1, 0, 0, 0)

    def to_x(g, pz, px, py):
        loop(nx - 1, lambda k: send(g, pz, px, py, 0, k + 1, 0, 0))

    def to_y(g, pz, px, py):
        loop(ny - 1, lambda k: send(g, pz, px, py, 0, 0, k + 1, 0))

    def to_core(g, pz, px, py):
        send(g, pz, px, py, 0, 0, 0, 1)

    tile = 256

    def multiply(g, start, depth, first=False):
        w = groups[g][0]
        acc = acca if g == "a" else accb
        k = pl.ds(pl.multiple_of(start, depth), depth)

        def at(i):
            cols = pl.ds(pl.multiple_of(i * tile, tile), tile)
            new = jnp.dot(feat[:, k], w[k, cols], preferred_element_type=jnp.float32)
            acc[:, cols] = new if first else acc[:, cols] + new

        loop(w.shape[1] // tile, at)

    def settle(g, pz, px, py):
        wait(g, pz, px, py, (c + 1) % CORES)

    def shard_of(g, pz, px):
        multiply(g, (pz * nx + px) * shard, shard)

    def sides(d, body):
        for up in (True, False):
            pz = z - d if up else z + d

            @pl.when(pz >= 0 if up else pz < nz)
            def _():
                body(pz, up)

    to_x("a", z, x, y)
    for g in ("b", "a"):
        to_z(g, z, True)
        to_z(g, z, False)
    loop(ny, lambda k: to_x("b", z, x, (y + k) % ny))

    def pass_b(pz, up):
        wait("b", pz, x, y, c)
        to_z("b", pz, up)
        to_y("b", pz, x, y)
        to_x("b", pz, x, y)
        to_core("b", pz, x, y)

    def pass_a(pz, up):
        wait("a", pz, x, y, c)
        to_z("a", pz, up)
        to_x("a", pz, x, y)
        to_y("a", pz, x, y)
        to_core("a", pz, x, y)

    def along_z(d):
        sides(d, pass_b)
        sides(d, pass_a)

    def second_a(pz):
        def go(k):
            px = (x + 1 + k) % nx
            wait("a", pz, px, y, c)
            to_y("a", pz, px, y)
            to_core("a", pz, px, y)

        loop(nx - 1, go)

    def second_b(pz):
        def go(k):
            py = (y + 1 + k) % ny
            wait("b", pz, x, py, c)
            to_x("b", pz, x, py)
            to_core("b", pz, x, py)

        loop(ny - 1, go)

    def settle_second(pz):
        loop(nx - 1, lambda k: settle("a", pz, (x + 1 + k) % nx, y))

    def settle_second_b(pz):
        loop(ny - 1, lambda k: settle("b", pz, x, (y + 1 + k) % ny))

    def third_b(body):
        loop((nx - 1) * ny, lambda k: body((x + 1 + k // ny) % nx, (y + k % ny) % ny))

    def third_a(body, skip):
        def go(k):
            k = k + skip
            body((x + k // (ny - 1)) % nx, (y + 1 + k % (ny - 1)) % ny)

        if ny > 1:
            loop(nx * (ny - 1) - skip, go)

    def take(g, pz):
        def go(px, py):
            wait(g, pz, px, py, c)
            to_core(g, pz, px, py)

        return go

    if nz > 1:
        along_z(1)
    second_a(z)
    fetch.wait()
    multiply("b", ti * shard, shard, True)
    multiply("a", ti * shard, shard, True)

    took(chain, tmn - 1, chain_recv)

    def back(k, state):
        carry, value_after = state
        at = tmn - 1 - k
        blk = chain[at]
        new = blk[1:2, 0:envs] + blk[2:3, 0:envs] * value_after + blk[0:1, 0:envs] * carry
        reached = at > ti
        return (
            jnp.where(reached, new, carry),
            jnp.where(reached, blk[3:4, 0:envs], value_after),
        )

    carry, value_after = lax.fori_loop(
        0, tmn, back, (jnp.zeros((1, envs), jnp.float32), last_ref[...])
    )
    advantage = base + tail * value_after + gain * carry
    stat[me, 0:1, 0:envs] = jnp.sum(advantage, axis=0, keepdims=True)
    stat[me, 1:2, 0:envs] = jnp.sum(advantage * advantage, axis=0, keepdims=True)
    norm_ref[...] = advantage
    tell_all(stat, stat_send, stat_recv)

    def middle(k):
        d = k + 1

        @pl.when(d + 1 < nz)
        def _():
            along_z(d + 1)

        def relay(pz, up):
            second_b(pz)
            second_a(pz)

        def near(pz, up):
            settle("b", pz, x, y)
            settle("a", pz, x, y)

        sides(d, relay)
        sides(d, near)

    loop(nz - 1, middle)
    third_b(take("b", z))
    third_a(take("a", z), ny - 1)
    settle_second(z)

    def last(k):
        def seconds(pz, up):
            settle_second_b(pz)
            shard_of("b", pz, x)
            settle_second(pz)

        def thirds(pz, up):
            third_b(take("b", pz))
            third_a(take("a", pz), 0)

        def close(pz, up):
            third_b(functools.partial(settle, "b", pz))
            loop(nx - 1, lambda k: shard_of("b", pz, (x + 1 + k) % nx))
            third_a(functools.partial(settle, "a", pz), 0)
            loop(nx, lambda k: shard_of("a", pz, (x + k) % nx))

        sides(k + 1, seconds)
        sides(k + 1, thirds)
        sides(k + 1, close)

    third_b(functools.partial(settle, "b", z))
    third_a(functools.partial(settle, "a", z), ny - 1)
    loop(nx - 1, lambda k: shard_of("b", z, (x + 1 + k) % nx))
    loop(nx - 1, lambda k: shard_of("a", z, (x + 1 + k) % nx))
    loop(nz - 1, last)

    took(stat, n - 1, stat_recv)
    count = rows * n
    adv_mean = jnp.sum(stat[:, 0:1, 0:envs]) / count
    adv_var = jnp.sum(stat[:, 1:2, 0:envs]) / count - adv_mean * adv_mean

    span = tile // envs

    def finish(i):
        r = pl.ds(pl.multiple_of(i * tile, tile), tile)
        t = pl.ds(pl.multiple_of(i * span, span), span)
        cube = (span, envs, envs)
        diag = lax.broadcasted_iota(jnp.int32, cube, 1) == lax.broadcasted_iota(jnp.int32, cube, 2)

        def square(col):
            return jnp.sum(jnp.where(diag, col.reshape(span, envs, 1), 0.0), axis=1)

        taken = act_ref[t, :]
        taken = jnp.sum(jnp.where(diag, taken[:, None, :], 0.0), axis=2, keepdims=True)
        taken = taken.reshape(tile, 1).astype(jnp.int32)
        logits = accb[r, ch : ch + acts]
        top = jnp.max(logits, axis=1, keepdims=True)
        total = jnp.sum(jnp.exp(logits - top), axis=1, keepdims=True)
        choose = lax.broadcasted_iota(jnp.int32, (tile, acts), 1) == taken
        picked = jnp.sum(jnp.where(choose, logits - top, 0.0), axis=1, keepdims=True)
        logp_ref[t, :] = square(picked - jnp.log(total))
        front = jnp.tanh(acca[r, :] + bias_ref[:, 0:ca]) * wv_ref[:, 0:ca]
        behind = jnp.tanh(accb[r, 0:ch] + bias_ref[:, ca:hid]) * wv_ref[:, ca:hid]
        value = jnp.sum(front, axis=1, keepdims=True) + jnp.sum(behind, axis=1, keepdims=True)
        value_ref[t, :] = square(value)

    loop(rows // tile, finish)

    advantage = norm_ref[...]
    norm = (advantage - adv_mean) / jnp.sqrt(jnp.full((1, 1), adv_var + 0.25))
    old = old_t[...].T
    value_pred = value_ref[...]
    ratio = jnp.exp(logp_ref[...] - olp_t[...].T)
    policy_term = -jnp.minimum(ratio * norm, jnp.clip(ratio, 0.8, 1.2) * norm)
    returns = advantage + old
    clipped = old + jnp.clip(value_pred - old, -0.2, 0.2)
    value_term = 0.5 * jnp.maximum((value_pred - returns) ** 2, (clipped - returns) ** 2)
    lsum[me, 0:1, 0:envs] = jnp.sum(policy_term, axis=0, keepdims=True)
    lsum[me, 1:2, 0:envs] = jnp.sum(value_term, axis=0, keepdims=True)
    tell_all(lsum, lsum_send, lsum_recv)
    norm_out[...] = norm.T
    value_out[...] = value_pred.T
    logp_out[...] = logp_ref[...].T

    sent_z = jnp.where(z + 1 < nz, z + 1, 0) + jnp.where(z > 0, nz - z, 0)
    to_partner = (nz * nx - 1) * ny
    sent_a = sent_z + (nx - 1) * nz + (nz * nx - 1) * (ny - 1) + to_partner
    sent_b = sent_z + (nx - 1) * nz * ny + (nz - 1) * (ny - 1) + to_partner

    def drain(g, count):
        w, _, out = groups[g]
        block = w.at[pl.ds(0, piece), :]
        lax.fori_loop(
            0, count, lambda k, _: (pltpu.make_async_copy(block, block, out).wait(), 0)[1], 0
        )

    drain("a", sent_a)
    drain("b", sent_b)
    took(chain, tmn - 1, chain_send)
    took(stat, n - 1, stat_send)
    took(lsum, n - 1, lsum_recv)
    loss_ref[0] = jnp.sum(lsum[:, 0:1, 0:envs]) / count
    loss_ref[1] = jnp.sum(lsum[:, 1:2, 0:envs]) / count
    took(lsum, n - 1, lsum_send)


def hand_over(norm, value, logp, loss, norm_out, value_out, logp_out, loss_out):
    norm_out[...] = norm[...]
    value_out[...] = value[...]
    logp_out[...] = logp[...]
    loss_out[0] = loss[0]
    loss_out[1] = loss[1]


def solution(mesh):
    tmn, envn = mesh.shape["tm"], mesh.shape["env"]

    def shards(
        features,
        w_hidden,
        b_hidden,
        w_value,
        w_policy,
        old_value,
        rewards,
        dones,
        discounts,
        last_value,
        actions,
        old_logprob,
    ):
        steps, envs, width = features.shape
        shard, hid = w_hidden.shape
        acts = w_policy.shape[1]
        rows = steps * envs
        n = tmn * envn
        ca = hid * 3 // 4
        cb = hid - ca + acts
        sizes = (tmn, envn, steps, envs, shard, hid, acts)
        cell = jax.ShapeDtypeStruct((envs, steps), jnp.float32)
        vmem = pl.BlockSpec(memory_space=pltpu.VMEM)
        dma = pltpu.SemaphoreType.DMA
        norm, value, logp, losses = pl.pallas_call(
            functools.partial(kernel, sizes),
            out_shape=(cell, cell, cell, jax.ShapeDtypeStruct((2,), jnp.float32)),
            in_specs=[pl.BlockSpec(memory_space=pl.ANY)] * 3 + [vmem] * 9,
            out_specs=(vmem, vmem, vmem, pl.BlockSpec(memory_space=pltpu.SMEM)),
            scratch_shapes=[pltpu.VMEM((steps, envs), jnp.float32)] * 4
            + [
                pltpu.VMEM((rows, width), jnp.bfloat16),
                pltpu.VMEM((width, ca), jnp.bfloat16),
                pltpu.VMEM((width, cb), jnp.bfloat16),
                pltpu.VMEM((rows, ca), jnp.float32),
                pltpu.VMEM((rows, cb), jnp.float32),
                pltpu.VMEM((tmn, 8, 128), jnp.float32),
                pltpu.VMEM((n, 8, 128), jnp.float32),
                pltpu.VMEM((n, 8, 128), jnp.float32),
                dma,
                dma((3,)),
                dma((n,)),
                dma((n,)),
                dma,
                dma,
                dma,
                dma,
                dma,
                dma,
                dma,
                dma,
            ],
            compiler_params=pltpu.CompilerParams(
                collective_id=0, has_side_effects=True, vmem_limit_bytes=60 * 1024 * 1024
            ),
        )(
            features.reshape(rows, width),
            w_hidden,
            w_policy,
            b_hidden.reshape(1, hid),
            w_value.reshape(1, hid),
            old_value.T,
            rewards.T,
            dones.T,
            discounts,
            last_value.reshape(1, envs),
            actions.T,
            old_logprob.T,
        )
        smem = pl.BlockSpec(memory_space=pltpu.SMEM)
        norm, value, logp, losses = pl.pallas_call(
            hand_over,
            out_shape=(cell, cell, cell, jax.ShapeDtypeStruct((2,), jnp.float32)),
            in_specs=[vmem, vmem, vmem, smem],
            out_specs=(vmem, vmem, vmem, smem),
        )(norm, value, logp, losses)
        return (norm.T, value.T, logp.T, losses)

    in_specs = (
        P("tm", "env", None),
        P("tm", None),
        P(),
        P(),
        P("tm", None),
        P("tm", "env"),
        P("tm", "env"),
        P("tm", "env"),
        P(None, "env"),
        P("env"),
        P("tm", "env"),
        P("tm", "env"),
    )
    out_specs = (P("tm", "env"), P("tm", "env"), P("tm", "env"), P())
    return jax.shard_map(shards, mesh=mesh, in_specs=in_specs, out_specs=out_specs, check_vma=False)
```

```python
import functools

import jax
import jax.numpy as jnp
from jax import lax
from jax.experimental import pallas as pl
from jax.experimental.pallas import tpu as pltpu
from jax.sharding import PartitionSpec as P

MESH = pl.DeviceIdType.MESH
CORES = 2


def along_x(tm):
    nx = 1
    while (2 * nx) * (2 * nx) <= tm and tm % (2 * nx) == 0:
        nx *= 2
    return nx


def loop(count, body):
    if count == 1:
        body(0)
    elif count > 1:
        lax.fori_loop(0, count, lambda i, _: (body(i), 0)[1], 0)


def later(x, s, fill):
    return jnp.concatenate([x[s:], jnp.full((s, x.shape[1]), fill, x.dtype)], 0)


def kernel(
    sizes,
    feat_hbm,
    wh_hbm,
    wp_hbm,
    bias_ref,
    wv_ref,
    old_t,
    rew_t,
    done_t,
    disc_ref,
    last_ref,
    act_t,
    olp_t,
    norm_out,
    value_out,
    logp_out,
    loss_ref,
    norm_ref,
    value_ref,
    logp_ref,
    act_ref,
    feat,
    wa,
    wb,
    acca,
    accb,
    chain,
    stat,
    lsum,
    feat_sem,
    w_sem,
    recva,
    recvb,
    senda,
    sendb,
    chain_send,
    chain_recv,
    stat_send,
    stat_recv,
    lsum_send,
    lsum_recv,
):
    tmn, envn, steps, envs, shard, hid, acts = sizes
    nx = along_x(tmn)
    nz = tmn // nx
    ny = envn // CORES
    piece = shard // envn
    rows = steps * envs
    ca = wa.shape[1]
    ch = hid - ca
    n = tmn * envn
    ti = lax.axis_index("tm")
    ei = lax.axis_index("env")
    z, x = ti // nx, ti % nx
    y, c = ei // CORES, ei % CORES
    me = ti * envn + ei

    loads = [
        pltpu.make_async_copy(
            wh_hbm.at[:, pl.ds(0, ca)], wa.at[pl.ds(ti * shard, shard), :], w_sem.at[0]
        ),
        pltpu.make_async_copy(
            wh_hbm.at[:, pl.ds(ca, ch)],
            wb.at[pl.ds(ti * shard, shard), pl.ds(0, ch)],
            w_sem.at[1],
        ),
        pltpu.make_async_copy(
            wp_hbm, wb.at[pl.ds(ti * shard, shard), pl.ds(ch, acts)], w_sem.at[2]
        ),
    ]
    for load in loads:
        load.start()
    fetch = pltpu.make_async_copy(feat_hbm, feat, feat_sem)
    fetch.start()

    barrier = pltpu.get_barrier_semaphore()

    def greet(k):
        other = (me + 1 + k) % n
        pl.semaphore_signal(
            barrier,
            inc=1,
            device_id={"tm": other // envn, "env": other % envn},
            device_id_type=MESH,
        )

    loop(n - 1, greet)

    keep = 1.0 - done_t[...].astype(jnp.float32).T
    old = old_t[...].T
    gamma = disc_ref[0:1, :]
    lam = disc_ref[1:2, :]
    row = lax.broadcasted_iota(jnp.int32, (steps, envs), 0)
    gain = (gamma * lam) * keep
    base = rew_t[...].T + gamma * keep * later(old, 1, 0.0) - old
    tail = jnp.where(row == steps - 1, gamma * keep, 0.0)
    s = 1
    while s < steps:
        base = base + gain * later(base, s, 0.0)
        tail = tail + gain * later(tail, s, 0.0)
        gain = gain * later(gain, s, 1.0)
        s *= 2
    act_ref[...] = act_t[...].astype(jnp.float32).T
    chain[ti, 0:1, 0:envs] = gain[0:1]
    chain[ti, 1:2, 0:envs] = base[0:1]
    chain[ti, 2:3, 0:envs] = tail[0:1]
    chain[ti, 3:4, 0:envs] = old[0:1]

    for load in loads:
        load.wait()
    pl.semaphore_wait(barrier, n - 1)

    def tell_chain(k):
        pltpu.make_async_remote_copy(
            src_ref=chain.at[ti],
            dst_ref=chain.at[ti],
            send_sem=chain_send,
            recv_sem=chain_recv,
            device_id={"tm": (ti + 1 + k) % tmn, "env": ei},
            device_id_type=MESH,
        ).start()

    loop(tmn - 1, tell_chain)

    def tell_all(buf, send_sem, recv_sem):
        def go(k):
            other = (me + 1 + k) % n
            pltpu.make_async_remote_copy(
                src_ref=buf.at[me],
                dst_ref=buf.at[me],
                send_sem=send_sem,
                recv_sem=recv_sem,
                device_id={"tm": other // envn, "env": other % envn},
                device_id_type=MESH,
            ).start()

        loop(n - 1, go)

    def took(buf, count, sem):
        pltpu.make_async_copy(buf.at[pl.ds(0, count)], buf.at[pl.ds(0, count)], sem).wait()

    def part(w, pz, px, py, pc):
        start = (pz * nx + px) * shard + (py * CORES + pc) * piece
        return w.at[pl.ds(pl.multiple_of(start, piece), piece), :]

    def slot(pz, px, py, pc):
        return (pz * nx + px) * envn + py * CORES + pc

    groups = {"a": (wa, recva, senda), "b": (wb, recvb, sendb)}

    def send(g, pz, px, py, dz, dx, dy, dc):
        w, recv, out = groups[g]
        block = part(w, pz, px, py, c)
        pltpu.make_async_remote_copy(
            src_ref=block,
            dst_ref=block,
            send_sem=out,
            recv_sem=recv.at[slot(pz, px, py, c)],
            device_id={
                "tm": ((z + dz) % nz) * nx + (x + dx) % nx,
                "env": ((y + dy) % ny) * CORES + (c + dc) % CORES,
            },
            device_id_type=MESH,
        ).start()

    def wait(g, pz, px, py, pc):
        w, recv, _ = groups[g]
        block = part(w, pz, px, py, pc)
        pltpu.make_async_copy(block, block, recv.at[slot(pz, px, py, pc)]).wait()

    def to_z(g, pz, up):
        there = z + 1 < nz if up else z > 0

        @pl.when(there)
        def _():
            send(g, pz, x, y, 1 if up else nz - 1, 0, 0, 0)

    def to_x(g, pz, px, py):
        loop(nx - 1, lambda k: send(g, pz, px, py, 0, k + 1, 0, 0))

    def to_y(g, pz, px, py):
        loop(ny - 1, lambda k: send(g, pz, px, py, 0, 0, k + 1, 0))

    def to_core(g, pz, px, py):
        send(g, pz, px, py, 0, 0, 0, 1)

    tile = 256

    def multiply(g, start, depth, first=False):
        w = groups[g][0]
        acc = acca if g == "a" else accb
        k = pl.ds(pl.multiple_of(start, depth), depth)

        def at(i):
            cols = pl.ds(pl.multiple_of(i * tile, tile), tile)
            new = jnp.dot(feat[:, k], w[k, cols], preferred_element_type=jnp.float32)
            acc[:, cols] = new if first else acc[:, cols] + new

        loop(w.shape[1] // tile, at)

    def settle(g, pz, px, py):
        wait(g, pz, px, py, (c + 1) % CORES)

    def shard_of(g, pz, px):
        multiply(g, (pz * nx + px) * shard, shard)

    def sides(d, body):
        for up in (True, False):
            pz = z - d if up else z + d

            @pl.when(pz >= 0 if up else pz < nz)
            def _():
                body(pz, up)

    to_x("a", z, x, y)
    for g in ("b", "a"):
        to_z(g, z, True)
        to_z(g, z, False)
    loop(ny, lambda k: to_x("b", z, x, (y + k) % ny))

    def pass_b(pz, up):
        wait("b", pz, x, y, c)
        to_z("b", pz, up)
        to_y("b", pz, x, y)
        to_x("b", pz, x, y)
        to_core("b", pz, x, y)

    def pass_a(pz, up):
        wait("a", pz, x, y, c)
        to_z("a", pz, up)
        to_x("a", pz, x, y)
        to_y("a", pz, x, y)
        to_core("a", pz, x, y)

    def along_z(d):
        sides(d, pass_b)
        sides(d, pass_a)

    def second_a(pz):
        def go(k):
            px = (x + 1 + k) % nx
            wait("a", pz, px, y, c)
            to_y("a", pz, px, y)
            to_core("a", pz, px, y)

        loop(nx - 1, go)

    def second_b(pz):
        def go(k):
            py = (y + 1 + k) % ny
            wait("b", pz, x, py, c)
            to_x("b", pz, x, py)
            to_core("b", pz, x, py)

        loop(ny - 1, go)

    def settle_second(pz):
        loop(nx - 1, lambda k: settle("a", pz, (x + 1 + k) % nx, y))

    def settle_second_b(pz):
        loop(ny - 1, lambda k: settle("b", pz, x, (y + 1 + k) % ny))

    def third_b(body):
        loop((nx - 1) * ny, lambda k: body((x + 1 + k // ny) % nx, (y + k % ny) % ny))

    def third_a(body, skip):
        def go(k):
            k = k + skip
            body((x + k // (ny - 1)) % nx, (y + 1 + k % (ny - 1)) % ny)

        if ny > 1:
            loop(nx * (ny - 1) - skip, go)

    def take(g, pz):
        def go(px, py):
            wait(g, pz, px, py, c)
            to_core(g, pz, px, py)

        return go

    if nz > 1:
        along_z(1)
    second_a(z)
    fetch.wait()
    multiply("b", ti * shard, shard, True)
    multiply("a", ti * shard, shard, True)

    took(chain, tmn - 1, chain_recv)

    def back(k, state):
        carry, value_after = state
        at = tmn - 1 - k
        blk = chain[at]
        new = blk[1:2, 0:envs] + blk[2:3, 0:envs] * value_after + blk[0:1, 0:envs] * carry
        reached = at > ti
        return (
            jnp.where(reached, new, carry),
            jnp.where(reached, blk[3:4, 0:envs], value_after),
        )

    carry, value_after = lax.fori_loop(
        0, tmn, back, (jnp.zeros((1, envs), jnp.float32), last_ref[...])
    )
    advantage = base + tail * value_after + gain * carry
    stat[me, 0:1, 0:envs] = jnp.sum(advantage, axis=0, keepdims=True)
    stat[me, 1:2, 0:envs] = jnp.sum(advantage * advantage, axis=0, keepdims=True)
    norm_ref[...] = advantage
    tell_all(stat, stat_send, stat_recv)

    def last(k):
        def seconds(pz, up):
            settle_second_b(pz)
            shard_of("b", pz, x)
            settle_second(pz)

        def thirds(pz, up):
            third_b(take("b", pz))
            third_a(take("a", pz), 0)

        def close(pz, up):
            third_b(functools.partial(settle, "b", pz))
            loop(nx - 1, lambda k: shard_of("b", pz, (x + 1 + k) % nx))
            third_a(functools.partial(settle, "a", pz), 0)
            loop(nx, lambda k: shard_of("a", pz, (x + k) % nx))

        sides(k + 1, seconds)
        sides(k + 1, thirds)
        sides(k + 1, close)

    def own_z():
        third_b(take("b", z))
        third_a(take("a", z), ny - 1)
        settle_second(z)
        third_b(functools.partial(settle, "b", z))
        third_a(functools.partial(settle, "a", z), ny - 1)
        loop(nx - 1, lambda k: shard_of("b", z, (x + 1 + k) % nx))
        loop(nx - 1, lambda k: shard_of("a", z, (x + 1 + k) % nx))

    def middle(k):
        d = k + 1

        @pl.when(d + 1 < nz)
        def _():
            along_z(d + 1)

        def relay(pz, up):
            second_b(pz)
            second_a(pz)

        def near(pz, up):
            settle("b", pz, x, y)
            settle("a", pz, x, y)

        sides(d, relay)
        sides(d, near)

        @pl.when(k == 0)
        def _():
            own_z()

        @pl.when(k >= 1)
        def _():
            last(k - 1)

    loop(nz - 1, middle)
    if nz - 1 <= 0:
        own_z()
    loop(min(1, nz - 1), lambda k: last(max(nz - 1 - 1, 0) + k))

    took(stat, n - 1, stat_recv)
    count = rows * n
    adv_mean = jnp.sum(stat[:, 0:1, 0:envs]) / count
    adv_var = jnp.sum(stat[:, 1:2, 0:envs]) / count - adv_mean * adv_mean

    span = tile // envs

    def finish(i):
        r = pl.ds(pl.multiple_of(i * tile, tile), tile)
        t = pl.ds(pl.multiple_of(i * span, span), span)
        cube = (span, envs, envs)
        diag = lax.broadcasted_iota(jnp.int32, cube, 1) == lax.broadcasted_iota(jnp.int32, cube, 2)

        def square(col):
            return jnp.sum(jnp.where(diag, col.reshape(span, envs, 1), 0.0), axis=1)

        taken = act_ref[t, :]
        taken = jnp.sum(jnp.where(diag, taken[:, None, :], 0.0), axis=2, keepdims=True)
        taken = taken.reshape(tile, 1).astype(jnp.int32)
        logits = accb[r, ch : ch + acts]
        top = jnp.max(logits, axis=1, keepdims=True)
        total = jnp.sum(jnp.exp(logits - top), axis=1, keepdims=True)
        choose = lax.broadcasted_iota(jnp.int32, (tile, acts), 1) == taken
        picked = jnp.sum(jnp.where(choose, logits - top, 0.0), axis=1, keepdims=True)
        logp_ref[t, :] = square(picked - jnp.log(total))
        front = jnp.tanh(acca[r, :] + bias_ref[:, 0:ca]) * wv_ref[:, 0:ca]
        behind = jnp.tanh(accb[r, 0:ch] + bias_ref[:, ca:hid]) * wv_ref[:, ca:hid]
        value = jnp.sum(front, axis=1, keepdims=True) + jnp.sum(behind, axis=1, keepdims=True)
        value_ref[t, :] = square(value)

    loop(rows // tile, finish)

    advantage = norm_ref[...]
    norm = (advantage - adv_mean) / jnp.sqrt(jnp.full((1, 1), adv_var + 0.25))
    old = old_t[...].T
    value_pred = value_ref[...]
    ratio = jnp.exp(logp_ref[...] - olp_t[...].T)
    policy_term = -jnp.minimum(ratio * norm, jnp.clip(ratio, 0.8, 1.2) * norm)
    returns = advantage + old
    clipped = old + jnp.clip(value_pred - old, -0.2, 0.2)
    value_term = 0.5 * jnp.maximum((value_pred - returns) ** 2, (clipped - returns) ** 2)
    lsum[me, 0:1, 0:envs] = jnp.sum(policy_term, axis=0, keepdims=True)
    lsum[me, 1:2, 0:envs] = jnp.sum(value_term, axis=0, keepdims=True)
    tell_all(lsum, lsum_send, lsum_recv)
    norm_out[...] = norm.T
    value_out[...] = value_pred.T
    logp_out[...] = logp_ref[...].T

    sent_z = jnp.where(z + 1 < nz, z + 1, 0) + jnp.where(z > 0, nz - z, 0)
    to_partner = (nz * nx - 1) * ny
    sent_a = sent_z + (nx - 1) * nz + (nz * nx - 1) * (ny - 1) + to_partner
    sent_b = sent_z + (nx - 1) * nz * ny + (nz - 1) * (ny - 1) + to_partner

    def drain(g, count):
        w, _, out = groups[g]
        block = w.at[pl.ds(0, piece), :]
        lax.fori_loop(
            0, count, lambda k, _: (pltpu.make_async_copy(block, block, out).wait(), 0)[1], 0
        )

    drain("a", sent_a)
    drain("b", sent_b)
    took(chain, tmn - 1, chain_send)
    took(stat, n - 1, stat_send)
    took(lsum, n - 1, lsum_recv)
    loss_ref[0] = jnp.sum(lsum[:, 0:1, 0:envs]) / count
    loss_ref[1] = jnp.sum(lsum[:, 1:2, 0:envs]) / count
    took(lsum, n - 1, lsum_send)


def hand_over(norm, value, logp, loss, norm_out, value_out, logp_out, loss_out):
    norm_out[...] = norm[...]
    value_out[...] = value[...]
    logp_out[...] = logp[...]
    loss_out[0] = loss[0]
    loss_out[1] = loss[1]


def solution(mesh):
    tmn, envn = mesh.shape["tm"], mesh.shape["env"]

    def shards(
        features,
        w_hidden,
        b_hidden,
        w_value,
        w_policy,
        old_value,
        rewards,
        dones,
        discounts,
        last_value,
        actions,
        old_logprob,
    ):
        steps, envs, width = features.shape
        shard, hid = w_hidden.shape
        acts = w_policy.shape[1]
        rows = steps * envs
        n = tmn * envn
        ca = hid * 3 // 4
        cb = hid - ca + acts
        sizes = (tmn, envn, steps, envs, shard, hid, acts)
        cell = jax.ShapeDtypeStruct((envs, steps), jnp.float32)
        vmem = pl.BlockSpec(memory_space=pltpu.VMEM)
        dma = pltpu.SemaphoreType.DMA
        norm, value, logp, losses = pl.pallas_call(
            functools.partial(kernel, sizes),
            out_shape=(cell, cell, cell, jax.ShapeDtypeStruct((2,), jnp.float32)),
            in_specs=[pl.BlockSpec(memory_space=pl.ANY)] * 3 + [vmem] * 9,
            out_specs=(vmem, vmem, vmem, pl.BlockSpec(memory_space=pltpu.SMEM)),
            scratch_shapes=[pltpu.VMEM((steps, envs), jnp.float32)] * 4
            + [
                pltpu.VMEM((rows, width), jnp.bfloat16),
                pltpu.VMEM((width, ca), jnp.bfloat16),
                pltpu.VMEM((width, cb), jnp.bfloat16),
                pltpu.VMEM((rows, ca), jnp.float32),
                pltpu.VMEM((rows, cb), jnp.float32),
                pltpu.VMEM((tmn, 8, 128), jnp.float32),
                pltpu.VMEM((n, 8, 128), jnp.float32),
                pltpu.VMEM((n, 8, 128), jnp.float32),
                dma,
                dma((3,)),
                dma((n,)),
                dma((n,)),
                dma,
                dma,
                dma,
                dma,
                dma,
                dma,
                dma,
                dma,
            ],
            compiler_params=pltpu.CompilerParams(
                collective_id=0, has_side_effects=True, vmem_limit_bytes=60 * 1024 * 1024
            ),
        )(
            features.reshape(rows, width),
            w_hidden,
            w_policy,
            b_hidden.reshape(1, hid),
            w_value.reshape(1, hid),
            old_value.T,
            rewards.T,
            dones.T,
            discounts,
            last_value.reshape(1, envs),
            actions.T,
            old_logprob.T,
        )
        smem = pl.BlockSpec(memory_space=pltpu.SMEM)
        norm, value, logp, losses = pl.pallas_call(
            hand_over,
            out_shape=(cell, cell, cell, jax.ShapeDtypeStruct((2,), jnp.float32)),
            in_specs=[vmem, vmem, vmem, smem],
            out_specs=(vmem, vmem, vmem, smem),
        )(norm, value, logp, losses)
        return (norm.T, value.T, logp.T, losses)

    in_specs = (
        P("tm", "env", None),
        P("tm", None),
        P(),
        P(),
        P("tm", None),
        P("tm", "env"),
        P("tm", "env"),
        P("tm", "env"),
        P(None, "env"),
        P("env"),
        P("tm", "env"),
        P("tm", "env"),
    )
    out_specs = (P("tm", "env"), P("tm", "env"), P("tm", "env"), P())
    return jax.shard_map(shards, mesh=mesh, in_specs=in_specs, out_specs=out_specs, check_vma=False)
```
